8 devices in a mesh: dp: 1 (over z), col: 2 (over y), row: 4 (over x, core).
Axes of the slice: x: 2, y: 2, z: 1, core: 2. Of those that a mesh axis runs over, the one named last changes fastest.
Arguments:
- seq_in: bfloat16 [128, 32, 2560], P(None, 'dp', 'row')
- w_in1: bfloat16 [2560, 10240], P('row', 'col')
- w_rec1: bfloat16 [2560, 10240], P('row', 'col')
- b_gate1: float32 [10240], P(('col', 'row'))
- w_in2: bfloat16 [2560, 10240], P('row', 'col')
- w_rec2: bfloat16 [2560, 10240], P('row', 'col')
- b_gate2: float32 [10240], P(('col', 'row'))
- h_init: float32 [2, 32, 2560], P(None, 'dp', 'row')
- c_init: float32 [2, 32, 2560], P(None, 'dp', 'row')
Outputs:
- output 1: bfloat16 [128, 32, 2560], P(None, 'dp', ('row', 'col'))
- output 2: float32 [32, 2560], P('dp', ('row', 'col'))
- output 3: float32 [32, 2560], P('dp', ('row', 'col'))
All inputs are finite; a program needn't handle non-finite values.
Results may differ from the reference program's by a relative error of at most 0.00360462.
Values are sent between devices in bfloat16 or wider.
A program may use at most 1 GiB of HBM per device.

```python
import jax
import jax.numpy as jnp
from jax import lax

HIDDEN = 2560
TIME_STEPS = 128
GROUP_BATCH = 32
ROW_SPLIT = 4
COL_SPLIT = 2


def forget_offset():
    unit_dev = HIDDEN // (ROW_SPLIT * COL_SPLIT)
    gate_index = (jnp.arange(4 * HIDDEN) // unit_dev) % 4
    return jnp.where(gate_index == 1, 1.0, 0.0).astype(jnp.float32)


def setup_inputs(seed: int = 0, part: int = 0) -> dict:
    shared_keys = jax.random.split(jax.random.key(seed), 6)
    part_keys = jax.random.split(jax.random.fold_in(jax.random.key(seed + 1), part), 3)
    w_scale = HIDDEN ** -0.5

    def weight_draw(rng_key):
        return (w_scale * jax.random.normal(rng_key, (HIDDEN, 4 * HIDDEN), jnp.float32)).astype(jnp.bfloat16)

    def bias_draw(rng_key):
        return 0.5 * jax.random.normal(rng_key, (4 * HIDDEN,), jnp.float32) + forget_offset()

    return {
        "seq_in": jax.random.normal(part_keys[0], (TIME_STEPS, GROUP_BATCH, HIDDEN), jnp.float32).astype(jnp.bfloat16),
        "w_in1": weight_draw(shared_keys[0]),
        "w_rec1": weight_draw(shared_keys[1]),
        "b_gate1": bias_draw(shared_keys[2]),
        "w_in2": weight_draw(shared_keys[3]),
        "w_rec2": weight_draw(shared_keys[4]),
        "b_gate2": bias_draw(shared_keys[5]),
        "h_init": 0.5 * jax.random.normal(part_keys[1], (2, GROUP_BATCH, HIDDEN), jnp.float32),
        "c_init": 1.2 * jax.random.normal(part_keys[2], (2, GROUP_BATCH, HIDDEN), jnp.float32),
    }


def lstm_layer(in_seq, w_in, w_rec, b_gate, h_first, c_first):
    batch_rows = in_seq.shape[1]
    unit_dev = HIDDEN // (ROW_SPLIT * COL_SPLIT)

    def to_packed(flat_state):
        return flat_state.reshape(batch_rows, ROW_SPLIT, COL_SPLIT, unit_dev).transpose(0, 2, 1, 3)

    def to_plain(packed_state):
        return packed_state.transpose(0, 2, 1, 3).reshape(batch_rows, HIDDEN)

    def lstm_step(carry_in, in_step):
        h_prev, c_prev = carry_in
        z_cols = jnp.dot(in_step, w_in, preferred_element_type=jnp.float32) + b_gate
        z_cols = z_cols + jnp.dot(h_prev, w_rec, preferred_element_type=jnp.float32)
        z_pack = z_cols.reshape(batch_rows, COL_SPLIT, ROW_SPLIT, 4, unit_dev)
        in_gate = jax.nn.sigmoid(z_pack[:, :, :, 0])
        forget = jax.nn.sigmoid(z_pack[:, :, :, 1])
        cell_in = jnp.tanh(z_pack[:, :, :, 2])
        out_gate = jax.nn.sigmoid(z_pack[:, :, :, 3])
        c_new = forget * c_prev + in_gate * cell_in
        h_new = to_plain(out_gate * jnp.tanh(c_new)).astype(jnp.bfloat16)
        return (h_new, c_new), h_new

    carry_out, h_seq = lax.scan(lstm_step, (h_first.astype(jnp.bfloat16), to_packed(c_first)), in_seq)
    return h_seq, to_plain(carry_out[1])


def reference(seq_in, w_in1, w_rec1, b_gate1, w_in2, w_rec2, b_gate2, h_init, c_init):
    h1_seq, c1_last = lstm_layer(seq_in, w_in1, w_rec1, b_gate1, h_init[0], c_init[0])
    h2_seq, c2_last = lstm_layer(h1_seq, w_in2, w_rec2, b_gate2, h_init[1], c_init[1])
    return h2_seq, c1_last, c2_last
```

```python
import jax
import jax.numpy as jnp
from jax import lax
from jax.experimental import pallas as pl
from jax.experimental.pallas import tpu as pltpu
from jax.sharding import PartitionSpec as P

MESH = pl.DeviceIdType.MESH
F32, BF16 = jnp.float32, jnp.bfloat16
LANES = 128
TILE = 256
STEPS, BATCH, HIDDEN = 128, 32, 2560
UNIT = 320
CHIP = 2 * UNIT
GATES = 4 * CHIP
TB = 4
NBLK = STEPS // TB
ROWS = TB * BATCH
LEAD = 3
NCHUNK = CHIP // LANES
MAIN = 2 * TILE
REST = CHIP - MAIN
CW = 4 * LANES
SHARE = ((0, 1, 2), (3, 4, 5), (6, 7), (8, 9))
PAD = 3 * LANES
FILL = 96
PARTNER, ACROSS, OVER = (0, 1, 0), (1, 0, 0), (1, 1, 0)
PEERS = ((1, 0, 1), (1, 0, 0), (0, 0, 1))
DIAG, NEXT_X, NEXT_Y = range(3)


def _roll_half(v):
    return pltpu.roll(v, LANES // 2, 1)


def _low_half(v):
    return lax.broadcasted_iota(jnp.int32, v.shape, 1) < LANES // 2


def _halves(get, first, second):
    if first % 2 == 0 and second == first + 1:
        return get(first // 2)
    lo, hi = get(first // 2), get(second // 2)
    lo = lo if first % 2 == 0 else _roll_half(lo)
    hi = hi if second % 2 == 1 else _roll_half(hi)
    return jnp.where(_low_half(lo), lo, hi)


def _repack(get, put):
    for chunk in range(NCHUNK):
        for gate in range(4):
            place = [20 * (u // 5) + 5 * gate + u % 5 for u in (2 * chunk, 2 * chunk + 1)]
            put(4 * chunk + gate, _halves(get, *place))


def _sigmoid(v):
    return 0.5 * jnp.tanh(0.5 * v) + 0.5


def _kernel(
    seq, w_in1, w_rec1, w_in2, w_rec2, bias, hc, h2_out, c1_out, c2_out, stage,
    win, wrec, a8, a4, zbuf, z, h8, h4, c_s, bias_s, braw, hcraw, out_own, out_far, size,
    w_recv, w_send, st_recv, st_send, fw_send, small_recv, small_send, seq_recv, seq_send, a_recv,
    h_recv, h_send, d_send, o_recv, o_send, c_recv, c_send,
):
    col, row = lax.axis_index("col"), lax.axis_index("row")
    x, core = row // 2, lax.rem(row, 2)

    def device(dx, dcore, dcol):
        px, pc, py = lax.rem(x + dx, 2), lax.rem(core + dcore, 2), lax.rem(col + dcol, 2)
        return {"col": py, "row": 2 * px + pc}

    def remote(src, dst, send, recv, to):
        return pltpu.make_async_remote_copy(
            src_ref=src, dst_ref=dst, send_sem=send, recv_sem=recv, device_id=device(*to), device_id_type=MESH
        )

    def arrived(ref, sem):
        pltpu.make_async_copy(ref, ref, sem).wait()

    def units_moved(units, sem):
        arrived(size.at[pl.ds(0, units // 8)], sem)

    barrier = pltpu.get_barrier_semaphore()
    others = [(dx, dc, dy) for dx in range(2) for dc in range(2) for dy in range(2) if dx + dc + dy]
    for to in others:
        pl.semaphore_signal(barrier, inc=1, device_id=device(*to), device_id_type=MESH)
    pl.semaphore_wait(barrier, len(others))

    own_cols = pl.ds(pl.multiple_of(x * GATES, GATES), GATES)
    far_cols = pl.ds(pl.multiple_of((1 - x) * GATES, GATES), GATES)

    def pieces(by_unit, src_core, half):
        start = half * UNIT
        unit = src_core * UNIT if by_unit else start
        whole = min(UNIT, MAIN - unit)
        out = [(start, whole, unit)]
        if whole < UNIT:
            out.append((start + whole, UNIT - whole, MAIN))
        return out

    def place(by_unit, cross, src_core, half, unit):
        group = cross + 2 * jnp.where(half == col, 0, 1) if by_unit else 2 * cross + src_core
        off = group * MAIN + unit if unit < MAIN else MAIN * 4 + group * REST
        return pl.multiple_of(off, 64)

    def w_copies(mat, by_unit, src_core, ref, cross, cols, buf, to, send_base):
        out = []
        for half in range(2):
            for i, (start, rows, unit) in enumerate(pieces(by_unit, src_core, half)):
                src = ref.at[pl.ds(start, rows), cols]
                dst = buf.at[pl.ds(place(by_unit, cross, src_core, half, unit), rows), :]
                recv = w_recv.at[mat, cross, src_core, half, i]
                if to is None:
                    out.append(pltpu.make_async_copy(src, dst, recv))
                else:
                    out.append(remote(src, dst, w_send.at[send_base + half, i], recv, to))
        return out

    def take_weights(buf, by_unit, mat, cross, src_core):
        for half in range(2):
            for i, (_, count, unit) in enumerate(pieces(by_unit, src_core, half)):
                off = place(by_unit, cross, src_core, half, unit)
                arrived(buf.at[pl.ds(off, count), :], w_recv.at[mat, cross, src_core, half, i])

                def group(g, carry):
                    rows = pl.ds(pl.multiple_of(off + g * 16, 16), 16)
                    tiles = [buf[rows, pl.ds(LANES * n, LANES)].astype(F32) for n in range(GATES // LANES)]

                    def put(n, v):
                        buf[rows, pl.ds(LANES * n, LANES)] = v.astype(BF16)

                    _repack(lambda n: tiles[n], put)
                    return carry

                lax.fori_loop(0, count // 16, group, 0)

    def tiles_of(buf8, buf4, at, ks):
        out = [buf8[at, k] if k < 8 else buf4[at, 2 * (k - 8) + i] for k in ks for i in range(1 if k < 8 else 2)]
        return jnp.concatenate(out, axis=1)

    def rows_of(weights, ks, j):
        cols = pl.ds(CW * j, CW)
        if list(ks) == list(range(ks[0], ks[0] + len(ks))):
            return weights[pl.ds(TILE * ks[0], TILE * len(ks)), cols]
        return jnp.concatenate([weights[pl.ds(TILE * k, TILE), cols] for k in ks], axis=0)

    def rec_dot(slot, ks, j):
        rows = jnp.concatenate([tiles_of(h8, h4, slot, ks), jnp.zeros((FILL, TILE * len(ks)), BF16)], axis=0)
        return jnp.dot(rows, rows_of(wrec, ks, j), preferred_element_type=F32)[:BATCH]

    def in_product(block, into, ks):
        for j in range(NCHUNK):
            cols = pl.ds(CW * j, CW)
            part = jnp.dot(tiles_of(a8, a4, block, ks), rows_of(win, ks, j), preferred_element_type=F32)
            if ks[0] == 0:
                zbuf[into, :, cols] = part + bias_s[0:1, cols]
            else:
                zbuf[into, :, cols] += part

    def put_h(slot, chunk, v):
        if chunk < 4:
            h8[slot, chunk // 2, :, pl.ds(LANES * (chunk % 2), LANES)] = v.astype(BF16)
        else:
            h4[slot, 0] = v.astype(BF16)

    def small_setup():
        for i in range(2):
            arrived(braw.at[i], small_recv.at[0, i])
            arrived(hcraw.at[i], small_recv.at[1, i])

        def put_bias(n, v):
            bias_s[:, pl.ds(LANES * n, LANES)] = v

        _repack(lambda n: braw[n // 10, :, pl.ds(LANES * (n % 10), LANES)], put_bias)
        for which in range(2):
            def get(n):
                return hcraw[n // 3, which, :, pl.ds(LANES * (n % 3), LANES)]

            for chunk in range(NCHUNK):
                v = _halves(get, *[u + u // 5 for u in (2 * chunk, 2 * chunk + 1)])
                if which == 0:
                    put_h(TB - 1, chunk, v)
                else:
                    c_s[:, pl.ds(LANES * chunk, LANES)] = v

    def split_units(get):
        near = [get(0), get(1), get(2)]
        a, b, c = (_roll_half(get(n)) for n in (2, 3, 4))
        return near, [jnp.where(_low_half(a), a, b), jnp.where(_low_half(b), b, c), c]

    def h_copy(slot, peer, part):
        to = PEERS[peer]
        rel = to[0] + 2 * to[2]
        if part < 2:
            src, dst = h8.at[slot, part], h8.at[slot, 2 * rel + part]
        else:
            src, dst = h4.at[slot, 0], h4.at[slot, rel]
        return remote(src, dst, h_send.at[slot], h_recv.at[slot, peer, part], to)

    def send_h(slot, part):
        for peer in range(3):
            h_copy(slot, peer, part).start()

    def h_sent(slot):
        units_moved(3 * CHIP, h_send.at[slot])

    def pass_on(block, s, slot):
        rows = pl.ds(BATCH * s, BATCH)
        return (
            remote(h8.at[slot], a8.at[block, :, rows, :], d_send.at[slot], a_recv.at[block], PARTNER),
            remote(h4.at[slot], a4.at[block, :, rows, :], d_send.at[slot], a_recv.at[block], PARTNER),
        )

    def passed_on(slot):
        units_moved(HIDDEN, d_send.at[slot])

    def seq_pieces(block, i, send):
        out = [remote(a8.at[block, i], a8.at[block, 4 + i], seq_send.at[send], a_recv.at[block], ACROSS)]
        if i < 2:
            out.append(remote(a4.at[block, i], a4.at[block, 2 + i], seq_send.at[send], a_recv.at[block], ACROSS))
        return out

    def seq_sent(i, send):
        units_moved(TB * (TILE + LANES if i < 2 else TILE), seq_send.at[send])

    def wait_block(layer, block):
        units_moved(TB * (HIDDEN if layer else HIDDEN // 2), a_recv.at[block])

    def out_copies(block, ring):
        return (
            pltpu.make_async_copy(out_own.at[ring], h2_out.at[block], o_send.at[ring, 0]),
            remote(out_far.at[ring], h2_out.at[block], o_send.at[ring, 1], o_recv, PARTNER),
        )

    def out_wait(block, ring):
        own, far = out_copies(block, ring)
        own.wait()
        far.wait_send()

    def one_step(layer, b, s):
        prev = (s + TB - 1) % TB
        ring = lax.rem(b, 2)
        nxt = jnp.minimum(b + 1, NBLK - 1)
        rows = pl.ds(BATCH * s, BATCH)

        def wait_for(*parts):
            for peer, part in parts:
                h_copy(prev, peer, part).wait_recv()

        for j in range(NCHUNK):
            cols = pl.ds(CW * j, CW)
            z[:, cols] = zbuf[ring, rows, cols] + rec_dot(prev, (0, 1), j)
        if s == 0:
            @pl.when(b + 1 < NBLK)
            def _():
                wait_block(layer, nxt)
        in_product(nxt, 1 - ring, SHARE[s])
        if layer == 0:
            @pl.when(b + LEAD < NBLK)
            def _():
                for cp in seq_pieces(jnp.minimum(b + LEAD, NBLK - 1), s, s):
                    cp.start()
        wait_for((NEXT_Y, 0), (NEXT_X, 0), (NEXT_Y, 1))
        for j in range(NCHUNK):
            z[:, pl.ds(CW * j, CW)] += rec_dot(prev, (4, 5, 2), j)
        wait_for((DIAG, 0), (NEXT_X, 1), (NEXT_Y, 2), (NEXT_X, 2), (DIAG, 1), (DIAG, 2))
        if layer == 0:
            if s == 0:
                @pl.when(b > 0)
                def _():
                    for cp in pass_on(jnp.maximum(b - 1, 0), TB - 1, prev):
                        cp.start()
            else:
                for cp in pass_on(b, s - 1, prev):
                    cp.start()
        if s == TB - 1:
            h_sent(s)
        else:
            pl.when(b > 0)(lambda: h_sent(s))
        if layer == 0:
            if s == TB - 1:
                passed_on(0)
            else:
                pl.when(b > 0)(lambda: passed_on((s + 1) % TB))
        if layer == 1 and s == 0:
            pl.when(b > 1)(lambda: out_wait(jnp.maximum(b - 2, 0), ring))

        new, part = [], []

        def products(*chunks):
            for j in chunks:
                part.append(rec_dot(prev, (6, 3, 7, 8, 9), j))

        def cell(j):
            units = pl.ds(LANES * j, LANES)
            zj = z[:, pl.ds(CW * j, CW)] + part[j]
            gates = [zj[:, LANES * m : LANES * (m + 1)] for m in range(4)]
            c_new = _sigmoid(gates[1]) * c_s[:, units] + _sigmoid(gates[0]) * jnp.tanh(gates[2])
            c_s[:, units] = c_new
            h_new = _sigmoid(gates[3]) * jnp.tanh(c_new)
            new.append(h_new)
            put_h(s, j, h_new)

        products(0, 1, 2)
        cell(0)
        cell(1)
        send_h(s, 0)
        products(3, 4)
        cell(2)
        cell(3)
        send_h(s, 1)
        cell(4)
        send_h(s, 2)
        if layer == 1:
            near, far = split_units(lambda n: new[n])
            for n in range(3):
                out_far[ring, rows, pl.ds(LANES * n, LANES)] = near[n].astype(BF16)
                out_own[ring, rows, pl.ds(LANES * n, LANES)] = far[n].astype(BF16)
            if s == TB - 1:
                for cp in out_copies(b, ring):
                    cp.start()

    def run_layer(layer):
        for ks in SHARE:
            in_product(0, 0, ks)

        def block(b, carry):
            if layer == 0:
                @pl.when((b > 0) & (b + LEAD - 1 < NBLK))
                def _():
                    for s in range(TB):
                        seq_sent(s, s)
            for s in range(TB):
                one_step(layer, b, s)
            return carry

        lax.fori_loop(0, NBLK, block, 0)
        slot = TB - 1
        for peer in range(3):
            for part in range(3):
                h_copy(slot, peer, part).wait_recv()
        if layer == 0:
            for cp in pass_on(NBLK - 1, slot, slot):
                cp.start()
            for s in (1, 2, 3):
                passed_on(s)
        for s in range(TB):
            h_sent(s)

    def begin():
        small_setup()
        for part in range(3):
            send_h(TB - 1, part)

    def end(keep, give, out, other):
        parts = split_units(lambda n: c_s[:, pl.ds(LANES * n, LANES)])
        for i in range(2):
            for n in range(3):
                hcraw[0, i, :, pl.ds(LANES * n, LANES)] = parts[i][n]
        kept = pltpu.make_async_copy(hcraw.at[0, keep], out, c_send.at[0])
        given = remote(hcraw.at[0, give], out, c_send.at[1], c_recv, PARTNER)
        kept.start()
        given.start()
        kept.wait()
        given.wait_send()
        arrived(other, c_recv)

    def seq_copies(group, rel, to, sems):
        out = []
        for i in range(3):
            src = seq.at[:, :, pl.ds(TILE * i, TILE if i < 2 else REST)]
            dst = a8.at[:, 2 * rel + i] if i < 2 else a4.at[:, rel]
            if to is None:
                out.append(pltpu.make_async_copy(src, dst, seq_recv.at[rel, i]))
            else:
                out.append(remote(src, dst, sems[i], seq_recv.at[rel, i], to))
        return out

    @pl.when(core == 0)
    def _():
        local = seq_copies(0, 0, None, None)
        local.append(pltpu.make_async_copy(bias.at[0], braw.at[0], small_recv.at[0, 0]))
        local.append(pltpu.make_async_copy(hc.at[0], hcraw.at[0], small_recv.at[1, 0]))
        local += w_copies(0, False, 0, w_in1, 0, own_cols, win, None, 0)
        local += w_copies(1, True, 0, w_rec1, 0, own_cols, wrec, None, 0)
        sent = [
            remote(bias.at[1], braw.at[0], small_send.at[0], small_recv.at[0, 0], PARTNER),
            remote(hc.at[1], hcraw.at[0], small_send.at[1], small_recv.at[1, 0], PARTNER),
            remote(w_in2.at[:, far_cols], stage.at[0], st_send.at[0], st_recv.at[0], PARTNER),
            remote(w_rec2.at[:, far_cols], stage.at[1], st_send.at[1], st_recv.at[1], PARTNER),
        ]
        sent += w_copies(0, True, 0, w_in2, 0, own_cols, win, PARTNER, 4)
        sent += w_copies(1, True, 0, w_rec2, 0, own_cols, wrec, PARTNER, 6)
        cross_in = w_copies(0, False, 0, w_in1, 1, far_cols, win, ACROSS, 0)
        cross_rec = w_copies(1, True, 0, w_rec1, 1, far_cols, wrec, ACROSS, 2)
        for cp in cross_in + local + sent:
            cp.start()
        for rel in range(2):
            for i in range(3):
                arrived(a8.at[:, 2 * rel + i] if i < 2 else a4.at[:, rel], seq_recv.at[rel, i])
        for b in range(LEAD):
            for i in range(TB):
                for cp in seq_pieces(b, i, TB + TB * b + i):
                    cp.start()
        for cp in cross_rec:
            cp.start()
        begin()
        for mat, buf in enumerate((win, wrec)):
            for cross in range(2):
                for src_core in range(2):
                    take_weights(buf, mat == 1, mat, cross, src_core)
        wait_block(0, 0)
        run_layer(0)
        end(0, 1, c1_out, c2_out)
        arrived(h2_out, o_recv)
        for b in range(LEAD):
            for i in range(TB):
                seq_sent(i, TB + TB * b + i)
        for cp in sent + cross_in + cross_rec:
            cp.wait_send()

    @pl.when(core == 1)
    def _():
        local = [
            pltpu.make_async_copy(bias.at[1], braw.at[1], small_recv.at[0, 1]),
            pltpu.make_async_copy(hc.at[1], hcraw.at[1], small_recv.at[1, 1]),
        ]
        local += w_copies(0, True, 1, w_in2, 0, own_cols, win, None, 0)
        local += w_copies(1, True, 1, w_rec2, 0, own_cols, wrec, None, 0)
        sent = seq_copies(0, 1, PARTNER, [small_send.at[2 + i] for i in range(3)])
        sent.append(remote(bias.at[0], braw.at[1], small_send.at[0], small_recv.at[0, 1], PARTNER))
        sent.append(remote(hc.at[0], hcraw.at[1], small_send.at[1], small_recv.at[1, 1], PARTNER))
        sent += w_copies(0, False, 1, w_in1, 1, far_cols, win, OVER, 0)
        sent += w_copies(1, True, 1, w_rec1, 1, far_cols, wrec, OVER, 2)
        sent += w_copies(0, False, 1, w_in1, 0, own_cols, win, PARTNER, 4)
        sent += w_copies(1, True, 1, w_rec1, 0, own_cols, wrec, PARTNER, 6)
        late_rec = w_copies(1, True, 1, w_rec2, 1, far_cols, wrec, ACROSS, 10)
        for cp in sent + local:
            cp.start()
        late = w_copies(0, True, 1, w_in2, 1, far_cols, win, ACROSS, 8)
        for mat, buf, more in ((0, win, late_rec), (1, wrec, [])):
            arrived(stage.at[mat], st_recv.at[mat])
            for half in range(2):
                rows = pl.ds(place(True, 1, 0, half, 0), UNIT)
                src = stage.at[mat, pl.ds(half * UNIT, UNIT), :]
                late.append(remote(src, buf.at[rows, :], fw_send.at[mat, half], w_recv.at[mat, 1, 0, half, 0], ACROSS))
            late += more
        for cp in late:
            cp.start()
        begin()
        for mat, buf in enumerate((win, wrec)):
            for cross in range(2):
                for src_core in (1, 0):
                    take_weights(buf, True, mat, cross, src_core)
        wait_block(1, 0)
        run_layer(1)
        for b in (NBLK - 2, NBLK - 1):
            out_wait(b, b % 2)
        end(1, 0, c2_out, c1_out)
        for cp in sent + late:
            cp.wait_send()


def solution(mesh):
    any_spec = pl.BlockSpec(memory_space=pl.ANY)
    dma = pltpu.SemaphoreType.DMA
    vmem = pltpu.VMEM

    def local_program(seq_in, w_in1, w_rec1, b_gate1, w_in2, w_rec2, b_gate2, h_init, c_init):
        col = lax.axis_index("col")
        states = jnp.stack([h_init, c_init], axis=1)
        states = lax.dynamic_slice_in_dim(states, col * UNIT, UNIT, axis=3)
        states = jnp.pad(states, ((0, 0), (0, 0), (0, 0), (0, PAD - UNIT)))
        bias = jnp.broadcast_to(jnp.stack([b_gate1, b_gate2])[:, None, :], (2, 8, 4 * UNIT))
        seq = seq_in.reshape(NBLK, ROWS, CHIP)
        h2, c1, c2, _ = pl.pallas_call(
            _kernel,
            out_shape=(
                jax.ShapeDtypeStruct((NBLK, ROWS, PAD), BF16),
                jax.ShapeDtypeStruct((BATCH, PAD), F32),
                jax.ShapeDtypeStruct((BATCH, PAD), F32),
                jax.ShapeDtypeStruct((2, CHIP, GATES), BF16),
            ),
            in_specs=[any_spec] * 7,
            out_specs=(any_spec,) * 4,
            scratch_shapes=[
                vmem((HIDDEN, GATES), BF16),
                vmem((HIDDEN, GATES), BF16),
                vmem((NBLK, 8, ROWS, TILE), BF16),
                vmem((NBLK, 4, ROWS, LANES), BF16),
                vmem((2, ROWS, GATES), F32),
                vmem((BATCH, GATES), F32),
                vmem((TB, 8, BATCH, TILE), BF16),
                vmem((TB, 4, BATCH, LANES), BF16),
                vmem((BATCH, CHIP), F32),
                vmem((8, GATES), F32),
                vmem((2, 8, 4 * UNIT), F32),
                vmem((2, 2, BATCH, PAD), F32),
                vmem((2, ROWS, PAD), BF16),
                vmem((2, ROWS, PAD), BF16),
                vmem((TB * HIDDEN // 8, LANES), F32),
                dma((2, 2, 2, 2, 2)),
                dma((12, 2)),
                dma((2,)),
                dma((2,)),
                dma((2, 2)),
                dma((2, 2)),
                dma((5,)),
                dma((2, 3)),
                dma((TB + TB * LEAD,)),
                dma((NBLK,)),
                dma((TB, 3, 3)),
                dma((TB,)),
                dma((TB,)),
                dma(()),
                dma((2, 2)),
                dma(()),
                dma((2,)),
            ],
            compiler_params=pltpu.CompilerParams(
                collective_id=0, has_side_effects=True, vmem_limit_bytes=62 * 2**20
            ),
        )(seq, w_in1, w_rec1, w_in2, w_rec2, bias, states)
        return h2.reshape(STEPS, BATCH, PAD)[:, :, :UNIT], c1[:, :UNIT], c2[:, :UNIT]

    row_spec = P(None, "dp", "row")
    weight_spec = P("row", "col")
    bias_spec = P(("col", "row"))
    seq_out_spec = P(None, "dp", ("row", "col"))
    cell_out_spec = P("dp", ("row", "col"))
    return jax.shard_map(
        local_program,
        mesh=mesh,
        in_specs=(row_spec, weight_spec, weight_spec, bias_spec, weight_spec, weight_spec, bias_spec, row_spec, row_spec),
        out_specs=(seq_out_spec, cell_out_spec, cell_out_spec),
        check_vma=False,
    )
```

```python
import jax
import jax.numpy as jnp
from jax import lax
from jax.experimental import pallas as pl
from jax.experimental.pallas import tpu as pltpu
from jax.sharding import PartitionSpec as P

MESH = pl.DeviceIdType.MESH
F32, BF16 = jnp.float32, jnp.bfloat16
LANES = 128
TILE = 256
STEPS, BATCH, HIDDEN = 128, 32, 2560
UNIT = 320
CHIP = 2 * UNIT
GATES = 4 * CHIP
TB = 4
NBLK = STEPS // TB
ROWS = TB * BATCH
LEAD = 3
DIRECT = ((0, 0),)
NCHUNK = CHIP // LANES
MAIN = 2 * TILE
REST = CHIP - MAIN
CW = 4 * LANES
SHARE = ((0, 1, 2), (3, 4, 5), (6, 7), (8, 9))
PAD = 3 * LANES
FILL = 96
PARTNER, ACROSS, OVER, ALONG = (0, 1, 0), (1, 0, 0), (1, 1, 0), (0, 0, 1)
PEERS = ((1, 0, 1), (1, 0, 0), (0, 0, 1))
DIAG, NEXT_X, NEXT_Y = range(3)


def _roll_half(v):
    return pltpu.roll(v, LANES // 2, 1)


def _low_half(v):
    return lax.broadcasted_iota(jnp.int32, v.shape, 1) < LANES // 2


def _halves(get, first, second):
    if first % 2 == 0 and second == first + 1:
        return get(first // 2)
    lo, hi = get(first // 2), get(second // 2)
    lo = lo if first % 2 == 0 else _roll_half(lo)
    hi = hi if second % 2 == 1 else _roll_half(hi)
    return jnp.where(_low_half(lo), lo, hi)


def _repack(get, put):
    for chunk in range(NCHUNK):
        for gate in range(4):
            place = [20 * (u // 5) + 5 * gate + u % 5 for u in (2 * chunk, 2 * chunk + 1)]
            put(4 * chunk + gate, _halves(get, *place))


def _sigmoid(v):
    return 0.5 * jnp.tanh(0.5 * v) + 0.5


def _kernel(
    seq, w_in1, w_rec1, w_in2, w_rec2, bias1, bias2, h_first, c_first, h2_out, c1_out, c2_out, stage,
    win, wrec, a8, a4, zbuf, z, h8, h4, c_s, bias_s, braw, hcraw, out_own, out_far, size,
    w_recv, w_send, st_recv, st_send, fw_send, small_recv, small_send, seq_recv, seq_send, a_recv,
    h_recv, h_send, d_send, o_recv, o_send, c_recv, c_send,
):
    col, row = lax.axis_index("col"), lax.axis_index("row")
    x, core = row // 2, lax.rem(row, 2)

    def device(dx, dcore, dcol):
        px, pc, py = lax.rem(x + dx, 2), lax.rem(core + dcore, 2), lax.rem(col + dcol, 2)
        return {"col": py, "row": 2 * px + pc}

    def remote(src, dst, send, recv, to):
        return pltpu.make_async_remote_copy(
            src_ref=src, dst_ref=dst, send_sem=send, recv_sem=recv, device_id=device(*to), device_id_type=MESH
        )

    def arrived(ref, sem):
        pltpu.make_async_copy(ref, ref, sem).wait()

    def units_moved(units, sem):
        arrived(size.at[pl.ds(0, units // 8)], sem)

    barrier = pltpu.get_barrier_semaphore()
    others = [(dx, dc, dy) for dx in range(2) for dc in range(2) for dy in range(2) if dx + dc + dy]
    for to in others:
        pl.semaphore_signal(barrier, inc=1, device_id=device(*to), device_id_type=MESH)
    pl.semaphore_wait(barrier, len(others))

    own_cols = pl.ds(pl.multiple_of(x * GATES, GATES), GATES)
    far_cols = pl.ds(pl.multiple_of((1 - x) * GATES, GATES), GATES)

    def pieces(by_unit, src_core, half):
        start = half * UNIT
        unit = src_core * UNIT if by_unit else start
        whole = min(UNIT, MAIN - unit)
        out = [(start, whole, unit)]
        if whole < UNIT:
            out.append((start + whole, UNIT - whole, MAIN))
        return out

    def place(by_unit, cross, src_core, half, unit):
        group = cross + 2 * jnp.where(half == col, 0, 1) if by_unit else 2 * cross + src_core
        off = group * MAIN + unit if unit < MAIN else MAIN * 4 + group * REST
        return pl.multiple_of(off, 64)

    def w_copies(mat, by_unit, src_core, ref, cross, cols, buf, to, send_base):
        out = []
        for half in range(2):
            for i, (start, rows, unit) in enumerate(pieces(by_unit, src_core, half)):
                src = ref.at[pl.ds(start, rows), cols]
                dst = buf.at[pl.ds(place(by_unit, cross, src_core, half, unit), rows), :]
                recv = w_recv.at[mat, cross, src_core, half, i]
                if to is None:
                    out.append(pltpu.make_async_copy(src, dst, recv))
                else:
                    out.append(remote(src, dst, w_send.at[send_base + half, i], recv, to))
        return out

    def take_weights(buf, by_unit, mat, cross, src_core):
        for half in range(2):
            for i, (_, count, unit) in enumerate(pieces(by_unit, src_core, half)):
                off = place(by_unit, cross, src_core, half, unit)
                arrived(buf.at[pl.ds(off, count), :], w_recv.at[mat, cross, src_core, half, i])

                def group(g, carry):
                    rows = pl.ds(pl.multiple_of(off + g * 16, 16), 16)
                    tiles = [buf[rows, pl.ds(LANES * n, LANES)].astype(F32) for n in range(GATES // LANES)]

                    def put(n, v):
                        buf[rows, pl.ds(LANES * n, LANES)] = v.astype(BF16)

                    _repack(lambda n: tiles[n], put)
                    return carry

                lax.fori_loop(0, count // 16, group, 0, unroll=4)

    def tiles_of(buf8, buf4, at, ks):
        out = [buf8[at, k] if k < 8 else buf4[at, 2 * (k - 8) + i] for k in ks for i in range(1 if k < 8 else 2)]
        return jnp.concatenate(out, axis=1)

    def rows_of(weights, ks, j):
        cols = pl.ds(CW * j, CW)
        if list(ks) == list(range(ks[0], ks[0] + len(ks))):
            return weights[pl.ds(TILE * ks[0], TILE * len(ks)), cols]
        return jnp.concatenate([weights[pl.ds(TILE * k, TILE), cols] for k in ks], axis=0)

    def rec_dot(slot, ks, j):
        rows = jnp.concatenate([tiles_of(h8, h4, slot, ks), jnp.zeros((FILL, TILE * len(ks)), BF16)], axis=0)
        return jnp.dot(rows, rows_of(wrec, ks, j), preferred_element_type=F32)[:BATCH]

    def in_product(block, into, ks):
        for j in range(NCHUNK):
            cols = pl.ds(CW * j, CW)
            part = jnp.dot(tiles_of(a8, a4, block, ks), rows_of(win, ks, j), preferred_element_type=F32)
            if ks[0] == 0:
                zbuf[into, :, cols] = part + bias_s[0:1, cols]
            else:
                zbuf[into, :, cols] += part

    def put_h(slot, chunk, v):
        if chunk < 4:
            h8[slot, chunk // 2, :, pl.ds(LANES * (chunk % 2), LANES)] = v.astype(BF16)
        else:
            h4[slot, 0] = v.astype(BF16)

    def small_setup():
        for src_core in range(2):
            for i, ref in enumerate((braw.at[src_core], hcraw.at[src_core, 0], hcraw.at[src_core, 1])):
                arrived(ref, small_recv.at[src_core, i])

        def get_bias(n):
            return jnp.broadcast_to(braw[n // 10, pl.ds(n % 10, 1), :], (8, LANES))

        def put_bias(n, v):
            bias_s[:, pl.ds(LANES * n, LANES)] = v

        _repack(get_bias, put_bias)
        for which in range(2):
            def get(n):
                return hcraw[n // NCHUNK, which, :, pl.ds(LANES * (n % NCHUNK), LANES)]

            for chunk in range(NCHUNK):
                blocks = [10 * (u // 5) + u % 5 for u in (2 * chunk, 2 * chunk + 1)]
                v = jnp.where(col == 0, _halves(get, *blocks), _halves(get, *[n + 5 for n in blocks]))
                if which == 0:
                    put_h(TB - 1, chunk, v)
                else:
                    c_s[:, pl.ds(LANES * chunk, LANES)] = v

    def small_copies(layer, src_core, to):
        refs = (
            ((bias1, bias2)[layer], braw.at[src_core]),
            (h_first.at[layer], hcraw.at[src_core, 0]),
            (c_first.at[layer], hcraw.at[src_core, 1]),
        )
        out = []
        for i, (src, dst) in enumerate(refs):
            recv = small_recv.at[src_core, i]
            if to is None:
                out.append(pltpu.make_async_copy(src, dst, recv))
            else:
                out.append(remote(src, dst, small_send.at[i], recv, to))
        return out

    def split_units(get):
        near = [get(0), get(1), get(2)]
        a, b, c = (_roll_half(get(n)) for n in (2, 3, 4))
        return near, [jnp.where(_low_half(a), a, b), jnp.where(_low_half(b), b, c), c]

    def h_copy(slot, peer, part):
        to = PEERS[peer]
        rel = to[0] + 2 * to[2]
        if part < 2:
            src, dst = h8.at[slot, part], h8.at[slot, 2 * rel + part]
        else:
            src, dst = h4.at[slot, 0], h4.at[slot, rel]
        return remote(src, dst, h_send.at[slot], h_recv.at[slot, peer, part], to)

    def send_h(slot, part):
        queue = (
            ((DIAG, 0), (NEXT_X, 0), (NEXT_Y, 0)),
            ((DIAG, 1), (NEXT_Y, 1)),
            ((DIAG, 2), (NEXT_X, 1), (NEXT_X, 2), (NEXT_Y, 2)),
        )
        for peer, piece in queue[part]:
            h_copy(slot, peer, piece).start()

    def h_sent(slot):
        units_moved(3 * CHIP, h_send.at[slot])

    def pass_on(block, s, slot):
        rows = pl.ds(BATCH * s, BATCH)
        return (
            remote(h8.at[slot], a8.at[block, :, rows, :], d_send.at[slot], a_recv.at[block], PARTNER),
            remote(h4.at[slot], a4.at[block, :, rows, :], d_send.at[slot], a_recv.at[block], PARTNER),
        )

    def passed_on(slot):
        units_moved(HIDDEN, d_send.at[slot])

    def seq_pieces(block, i, send, hand_on):
        first, to = (1, ALONG) if hand_on else (0, ACROSS)
        bufs = ((a8, 4 * first + i, 4 + i), (a4, 2 * first + i, 2 + i))
        return [
            remote(buf.at[block, src], buf.at[block, dst], seq_send.at[send], a_recv.at[block], to)
            for buf, src, dst in bufs[: 2 if i < 2 else 1]
        ]

    def crosses_here(block):
        return lax.rem(block + col, 2) == 0

    def seq_step(b, s):
        ahead, behind = b + LEAD + 1, b + LEAD

        @pl.when(crosses_here(ahead) & (ahead < NBLK))
        def _():
            for cp in seq_pieces(jnp.minimum(ahead, NBLK - 1), s, s, False):
                cp.start()

        @pl.when(crosses_here(behind) & (behind < NBLK))
        def _():
            block = jnp.minimum(behind, NBLK - 1)
            if s == 0:
                block_arrived(0, block)
            for cp in seq_pieces(block, s, s, True):
                cp.start()

    def seq_sent(i, send):
        units_moved(TB * (TILE + LANES if i < 2 else TILE), seq_send.at[send])

    def block_arrived(layer, block):
        units_moved(TB * (HIDDEN if layer else HIDDEN // 2), a_recv.at[block])

    def wait_block(layer, block):
        if layer == 0:
            pl.when(jnp.logical_not(crosses_here(block)))(lambda: block_arrived(layer, block))
        else:
            block_arrived(layer, block)

    def out_copies(block, ring):
        return (
            pltpu.make_async_copy(out_own.at[ring], h2_out.at[block], o_send.at[ring, 0]),
            remote(out_far.at[ring], h2_out.at[block], o_send.at[ring, 1], o_recv, PARTNER),
        )

    def out_wait(block, ring):
        own, far = out_copies(block, ring)
        own.wait()
        far.wait_send()

    def one_step(layer, b, s):
        prev = (s + TB - 1) % TB
        ring = lax.rem(b, 2)
        nxt = jnp.minimum(b + 1, NBLK - 1)
        rows = pl.ds(BATCH * s, BATCH)

        def wait_for(*parts):
            for peer, part in parts:
                h_copy(prev, peer, part).wait_recv()

        if s == TB - 1:
            h_sent(s)
        else:
            pl.when(b > 0)(lambda: h_sent(s))
        if layer == 0:
            if s == TB - 1:
                passed_on(0)
            else:
                pl.when(b > 0)(lambda: passed_on((s + 1) % TB))
        if layer == 1 and s == 0:
            pl.when(b > 1)(lambda: out_wait(jnp.maximum(b - 2, 0), ring))
        for j in range(NCHUNK):
            cols = pl.ds(CW * j, CW)
            z[:, cols] = zbuf[ring, rows, cols] + rec_dot(prev, (0, 1), j)
        if s == 0:
            @pl.when(b + 1 < NBLK)
            def _():
                wait_block(layer, nxt)
        in_product(nxt, 1 - ring, SHARE[s])
        if layer == 0:
            seq_step(b, s)

        def add(*ks):
            for j in range(NCHUNK):
                z[:, pl.ds(CW * j, CW)] += rec_dot(prev, ks, j)

        wait_for((NEXT_Y, 0))
        add(4)
        wait_for((NEXT_X, 0), (NEXT_Y, 1))
        add(2, 5)
        wait_for((DIAG, 0), (NEXT_Y, 2), (NEXT_X, 1), (NEXT_X, 2), (DIAG, 1), (DIAG, 2))
        new, part = [], []

        def products(*chunks):
            for j in chunks:
                part.append(rec_dot(prev, (3, 6, 7, 8, 9), j))

        def cell(j):
            units = pl.ds(LANES * j, LANES)
            zj = z[:, pl.ds(CW * j, CW)] + part[j]
            gates = [zj[:, LANES * m : LANES * (m + 1)] for m in range(4)]
            c_new = _sigmoid(gates[1]) * c_s[:, units] + _sigmoid(gates[0]) * jnp.tanh(gates[2])
            c_s[:, units] = c_new
            h_new = _sigmoid(gates[3]) * jnp.tanh(c_new)
            new.append(h_new)
            put_h(s, j, h_new)

        products(0, 1, 2)
        cell(0)
        cell(1)
        send_h(s, 0)
        products(3, 4)
        cell(2)
        cell(3)
        send_h(s, 1)
        cell(4)
        send_h(s, 2)
        if layer == 0:
            if s == 0:
                @pl.when(b > 0)
                def _():
                    for cp in pass_on(jnp.maximum(b - 1, 0), TB - 1, prev):
                        cp.start()
            else:
                for cp in pass_on(b, s - 1, prev):
                    cp.start()
        if layer == 1:
            near, far = split_units(lambda n: new[n])
            for n in range(3):
                out_far[ring, rows, pl.ds(LANES * n, LANES)] = near[n].astype(BF16)
                out_own[ring, rows, pl.ds(LANES * n, LANES)] = far[n].astype(BF16)
            if s == TB - 1:
                for cp in out_copies(b, ring):
                    cp.start()

    def take_all(buf, layer, mat):
        for cross in range(2):
            for src_core in (1, 0):
                take_weights(buf, layer == 1 or mat == 1, mat, cross, src_core)

    def first_input():
        for ks in SHARE:
            in_product(0, 0, ks)

    def run_layer(layer):
        def block(b, carry):
            if layer == 0:
                last = jnp.where(crosses_here(b + LEAD), NBLK - LEAD, NBLK - LEAD + 1)

                @pl.when((b > 0) & (b < last))
                def _():
                    for s in range(TB):
                        seq_sent(s, s)
            for s in range(TB):
                one_step(layer, b, s)
            return carry

        lax.fori_loop(0, NBLK, block, 0)

    def leave_exchange(layer):
        slot = TB - 1
        for peer in range(3):
            for part in range(3):
                h_copy(slot, peer, part).wait_recv()
        if layer == 0:
            for cp in pass_on(NBLK - 1, slot, slot):
                cp.start()
            for s in (1, 2, 3):
                passed_on(s)
        for s in range(TB):
            h_sent(s)

    def begin():
        small_setup()
        for part in range(3):
            send_h(TB - 1, part)

    def end(keep, give, out, other):
        parts = split_units(lambda n: c_s[:, pl.ds(LANES * n, LANES)])
        for i in range(2):
            for n in range(3):
                hcraw[0, i, :, pl.ds(LANES * n, LANES)] = parts[i][n]
        wide = pl.ds(0, PAD)
        kept = pltpu.make_async_copy(hcraw.at[0, keep, :, wide], out, c_send.at[0])
        given = remote(hcraw.at[0, give, :, wide], out, c_send.at[1], c_recv, PARTNER)
        kept.start()
        given.start()
        kept.wait()
        given.wait_send()
        arrived(other, c_recv)

    def seq_copies(group, rel, to, sems):
        out = []
        for i in range(3):
            src = seq.at[:, :, pl.ds(TILE * i, TILE if i < 2 else REST)]
            dst = a8.at[:, 2 * rel + i] if i < 2 else a4.at[:, rel]
            if to is None:
                out.append(pltpu.make_async_copy(src, dst, seq_recv.at[rel, i]))
            else:
                out.append(remote(src, dst, sems[i], seq_recv.at[rel, i], to))
        return out

    @pl.when(core == 0)
    def _():
        local = seq_copies(0, 0, None, None)
        local += small_copies(0, 0, None)
        local += w_copies(0, False, 0, w_in1, 0, own_cols, win, None, 0)
        local += w_copies(1, True, 0, w_rec1, 0, own_cols, wrec, None, 0)
        sent = small_copies(1, 0, PARTNER)
        more = []
        for mat, ref, buf in ((0, w_in2, win), (1, w_rec2, wrec)):
            for half in range(2):
                rows = pl.ds(half * UNIT, UNIT)
                if (mat, half) in DIRECT:
                    dst = buf.at[pl.ds(place(True, 1, 0, half, 0), UNIT), :]
                    recv = w_recv.at[mat, 1, 0, half, 0]
                    more.append(remote(ref.at[rows, far_cols], dst, st_send.at[mat, half], recv, OVER))
                else:
                    dst, recv = stage.at[mat, rows, :], st_recv.at[mat, half]
                    sent.append(remote(ref.at[rows, far_cols], dst, st_send.at[mat, half], recv, PARTNER))
        sent += w_copies(0, True, 0, w_in2, 0, own_cols, win, PARTNER, 4)
        sent += w_copies(1, True, 0, w_rec2, 0, own_cols, wrec, PARTNER, 6)
        cross_in = w_copies(0, False, 0, w_in1, 1, far_cols, win, ACROSS, 0)
        cross_rec = w_copies(1, True, 0, w_rec1, 1, far_cols, wrec, ACROSS, 2)
        for cp in cross_in + local + sent:
            cp.start()
        for rel in range(2):
            for i in range(3):
                arrived(a8.at[:, 2 * rel + i] if i < 2 else a4.at[:, rel], seq_recv.at[rel, i])
        for n in range(2):
            for i in range(TB):
                for cp in seq_pieces(col + 2 * n, i, TB * (n + 1) + i, False):
                    cp.start()
        for cp in cross_rec:
            cp.start()
        begin()
        for cp in more:
            cp.start()

        def hand_on(n):
            block_arrived(0, col + 2 * n)
            for i in range(TB):
                for cp in seq_pieces(col + 2 * n, i, TB * (n + 3) + i, True):
                    cp.start()

        hand_on(0)
        pl.when(col == 0)(lambda: hand_on(1))
        take_all(win, 0, 0)
        wait_block(0, 0)
        first_input()
        take_all(wrec, 0, 1)
        run_layer(0)
        leave_exchange(0)
        end(0, 1, c1_out, c2_out)
        arrived(h2_out, o_recv)
        for n in range(3):
            for i in range(TB):
                seq_sent(i, TB * (n + 1) + i)

        @pl.when(col == 0)
        def _():
            for i in range(TB):
                seq_sent(i, 4 * TB + i)

        for cp in sent + cross_in + cross_rec + more:
            cp.wait_send()

    @pl.when(core == 1)
    def _():
        local = small_copies(1, 1, None)
        local += w_copies(0, True, 1, w_in2, 0, own_cols, win, None, 0)
        local += w_copies(1, True, 1, w_rec2, 0, own_cols, wrec, None, 0)
        sent = seq_copies(0, 1, PARTNER, [small_send.at[3 + i] for i in range(3)])
        sent += small_copies(0, 1, PARTNER)
        sent += w_copies(0, False, 1, w_in1, 1, far_cols, win, OVER, 0)
        sent += w_copies(1, True, 1, w_rec1, 1, far_cols, wrec, OVER, 2)
        sent += w_copies(0, False, 1, w_in1, 0, own_cols, win, PARTNER, 4)
        sent += w_copies(1, True, 1, w_rec1, 0, own_cols, wrec, PARTNER, 6)
        late_rec = w_copies(1, True, 1, w_rec2, 1, far_cols, wrec, ACROSS, 10)
        for cp in sent + local:
            cp.start()
        late = w_copies(0, True, 1, w_in2, 1, far_cols, win, ACROSS, 8)
        for mat, buf, more in ((0, win, late_rec), (1, wrec, [])):
            for half in range(2):
                if (mat, half) not in DIRECT:
                    rows = pl.ds(place(True, 1, 0, half, 0), UNIT)
                    src = stage.at[mat, pl.ds(half * UNIT, UNIT), :]
                    arrived(src, st_recv.at[mat, half])
                    recv = w_recv.at[mat, 1, 0, half, 0]
                    late.append(remote(src, buf.at[rows, :], fw_send.at[mat, half], recv, ACROSS))
            late += more
        for cp in late:
            cp.start()
        begin()
        take_all(win, 1, 0)
        wait_block(1, 0)
        first_input()
        take_all(wrec, 1, 1)
        run_layer(1)
        end(1, 0, c2_out, c1_out)
        for b in (NBLK - 2, NBLK - 1):
            out_wait(b, b % 2)
        leave_exchange(1)
        for cp in sent + late:
            cp.wait_send()


def _trim(c1_in, c2_in, c1_out, c2_out):
    c1_out[...] = c1_in[:, :UNIT]
    c2_out[...] = c2_in[:, :UNIT]


def solution(mesh):
    any_spec = pl.BlockSpec(memory_space=pl.ANY)
    dma = pltpu.SemaphoreType.DMA
    vmem = pltpu.VMEM

    def local_program(seq_in, w_in1, w_rec1, b_gate1, w_in2, w_rec2, b_gate2, h_init, c_init):
        seq = seq_in.reshape(NBLK, ROWS, CHIP)
        h2, c1, c2, _ = pl.pallas_call(
            _kernel,
            out_shape=(
                jax.ShapeDtypeStruct((NBLK, ROWS, PAD), BF16),
                jax.ShapeDtypeStruct((BATCH, PAD), F32),
                jax.ShapeDtypeStruct((BATCH, PAD), F32),
                jax.ShapeDtypeStruct((2, CHIP, GATES), BF16),
            ),
            in_specs=[any_spec] * 9,
            out_specs=(any_spec,) * 4,
            scratch_shapes=[
                vmem((HIDDEN, GATES), BF16),
                vmem((HIDDEN, GATES), BF16),
                vmem((NBLK, 8, ROWS, TILE), BF16),
                vmem((NBLK, 4, ROWS, LANES), BF16),
                vmem((2, ROWS, GATES), F32),
                vmem((BATCH, GATES), F32),
                vmem((TB, 8, BATCH, TILE), BF16),
                vmem((TB, 4, BATCH, LANES), BF16),
                vmem((BATCH, CHIP), F32),
                vmem((8, GATES), F32),
                vmem((2, 4 * UNIT // LANES, LANES), F32),
                vmem((2, 2, BATCH, CHIP), F32),
                vmem((2, ROWS, PAD), BF16),
                vmem((2, ROWS, PAD), BF16),
                vmem((TB * HIDDEN // 8, LANES), F32),
                dma((2, 2, 2, 2, 2)),
                dma((12, 2)),
                dma((2, 2)),
                dma((2, 2)),
                dma((2, 2)),
                dma((2, 3)),
                dma((6,)),
                dma((2, 3)),
                dma((5 * TB,)),
                dma((NBLK,)),
                dma((TB, 3, 3)),
                dma((TB,)),
                dma((TB,)),
                dma(()),
                dma((2, 2)),
                dma(()),
                dma((2,)),
            ],
            compiler_params=pltpu.CompilerParams(
                collective_id=0, has_side_effects=True, vmem_limit_bytes=62 * 2**20
            ),
        )(seq, w_in1, w_rec1, w_in2, w_rec2, b_gate1.reshape(-1, LANES), b_gate2.reshape(-1, LANES), h_init, c_init)
        cell = jax.ShapeDtypeStruct((BATCH, UNIT), F32)
        c1, c2 = pl.pallas_call(_trim, out_shape=(cell, cell))(c1, c2)
        return h2.reshape(STEPS, BATCH, PAD)[:, :, :UNIT], c1, c2

    row_spec = P(None, "dp", "row")
    weight_spec = P("row", "col")
    bias_spec = P(("col", "row"))
    seq_out_spec = P(None, "dp", ("row", "col"))
    cell_out_spec = P("dp", ("row", "col"))
    return jax.shard_map(
        local_program,
        mesh=mesh,
        in_specs=(row_spec, weight_spec, weight_spec, bias_spec, weight_spec, weight_spec, bias_spec, row_spec, row_spec),
        out_specs=(seq_out_spec, cell_out_spec, cell_out_spec),
        check_vma=False,
    )
```

```python
import jax
import jax.numpy as jnp
from jax import lax
from jax.experimental import pallas as pl
from jax.experimental.pallas import tpu as pltpu
from jax.sharding import PartitionSpec as P

MESH = pl.DeviceIdType.MESH
F32, BF16 = jnp.float32, jnp.bfloat16
LANES = 128
TILE = 256
NTILE = 10
STEPS, BATCH, HIDDEN = 128, 32, 2560
UNIT = 320
CHIP = 2 * UNIT
GATES = 4 * CHIP
TB = 4
NBLK = STEPS // TB
ROWS = TB * BATCH
LEAD = 3
DIRECT = ((0, 0), (0, 1))
NCHUNK = CHIP // LANES
MAIN = 2 * TILE
REST = CHIP - MAIN
CW = 4 * LANES
SHARE = ((0, 1, 2), (3, 4, 5), (6, 7), (8, 9))
HALVES = (range(5), range(5, NTILE))
PAIR = 2 * BATCH
BOTH = range(2)
SQUARE = (2, 2)
PAD = 3 * LANES
FILL = 96
PARTNER, ACROSS, OVER, ALONG = (0, 1, 0), (1, 0, 0), (1, 1, 0), (0, 0, 1)
PEERS = ((1, 0, 1), (1, 0, 0), (0, 0, 1))
DIAG, NEXT_X, NEXT_Y = range(3)


def _roll_half(v):
    return pltpu.roll(v, LANES // 2, 1)


def _low_half(v):
    return lax.broadcasted_iota(jnp.int32, v.shape, 1) < LANES // 2


def _halves(get, first, second):
    if first % 2 == 0 and second == first + 1:
        return get(first // 2)
    lo, hi = get(first // 2), get(second // 2)
    lo = lo if first % 2 == 0 else _roll_half(lo)
    hi = hi if second % 2 == 1 else _roll_half(hi)
    return jnp.where(_low_half(lo), lo, hi)


def _repack(get, put):
    for chunk in range(NCHUNK):
        for gate in range(4):
            place = [20 * (u // 5) + 5 * gate + u % 5 for u in (2 * chunk, 2 * chunk + 1)]
            put(4 * chunk + gate, _halves(get, *place))


def _sigmoid(v):
    return 0.5 * jnp.tanh(0.5 * v) + 0.5


def _kernel(
    seq, w_in1, w_rec1, w_in2, w_rec2, bias1, bias2, h_first, c_first, h2_out, c1_out, c2_out, stage,
    win, wrec, a8, a4, zbuf, z, h8, h4, c_s, bias_s, braw, hcraw, out_own, out_far, size,
    w_recv, w_send, st_recv, st_send, fw_send, small_recv, small_send, seq_recv, seq_send, a_recv,
    h_recv, h_send, d_send, o_recv, o_send, c_recv, c_send,
):
    col, row = lax.axis_index("col"), lax.axis_index("row")
    x, core = row // 2, lax.rem(row, 2)

    def device(dx, dcore, dcol):
        px, pc, py = lax.rem(x + dx, 2), lax.rem(core + dcore, 2), lax.rem(col + dcol, 2)
        return {"col": py, "row": 2 * px + pc}

    def remote(src, dst, send, recv, to):
        return pltpu.make_async_remote_copy(
            src_ref=src, dst_ref=dst, send_sem=send, recv_sem=recv, device_id=device(*to), device_id_type=MESH
        )

    def arrived(ref, sem):
        pltpu.make_async_copy(ref, ref, sem).wait()

    def units_moved(units, sem):
        arrived(size.at[pl.ds(0, units // 8)], sem)

    barrier = pltpu.get_barrier_semaphore()
    others = [(dx, dc, dy) for dx in BOTH for dc in BOTH for dy in BOTH if dx + dc + dy]
    for to in others:
        pl.semaphore_signal(barrier, inc=1, device_id=device(*to), device_id_type=MESH)
    pl.semaphore_wait(barrier, len(others))

    own_cols = pl.ds(pl.multiple_of(x * GATES, GATES), GATES)
    far_cols = pl.ds(pl.multiple_of((1 - x) * GATES, GATES), GATES)

    def pieces(by_unit, src_core, half):
        start = half * UNIT
        unit = src_core * UNIT if by_unit else start
        whole = min(UNIT, MAIN - unit)
        out = [(start, whole, unit)]
        if whole < UNIT:
            out.append((start + whole, UNIT - whole, MAIN))
        return out

    def place(by_unit, cross, src_core, half, unit):
        group = cross + 2 * jnp.where(half == col, 0, 1) if by_unit else 2 * cross + src_core
        off = group * MAIN + unit if unit < MAIN else MAIN * 4 + group * REST
        return pl.multiple_of(off, 64)

    def w_copies(mat, by_unit, src_core, ref, cross, cols, buf, to, send_base):
        out = []
        for half in BOTH:
            for i, (start, rows, unit) in enumerate(pieces(by_unit, src_core, half)):
                src = ref.at[pl.ds(start, rows), cols]
                dst = buf.at[pl.ds(place(by_unit, cross, src_core, half, unit), rows), :]
                recv = w_recv.at[mat, cross, src_core, half, i]
                if to is None:
                    out.append(pltpu.make_async_copy(src, dst, recv))
                else:
                    out.append(remote(src, dst, w_send.at[send_base + half, i], recv, to))
        return out

    def take_weights(buf, by_unit, mat, cross, src_core):
        for half in BOTH:
            for i, (_, count, unit) in enumerate(pieces(by_unit, src_core, half)):
                off = place(by_unit, cross, src_core, half, unit)
                arrived(buf.at[pl.ds(off, count), :], w_recv.at[mat, cross, src_core, half, i])

                def group(g, carry):
                    rows = pl.ds(pl.multiple_of(off + g * 16, 16), 16)
                    tiles = [buf[rows, pl.ds(LANES * n, LANES)].astype(F32) for n in range(GATES // LANES)]

                    def put(n, v):
                        buf[rows, pl.ds(LANES * n, LANES)] = v.astype(BF16)

                    _repack(lambda n: tiles[n], put)
                    return carry

                lax.fori_loop(0, count // 16, group, 0, unroll=4)

    def tiles_of(buf8, buf4, at, ks):
        out = [buf8[at, k] if k < 8 else buf4[at, 2 * (k - 8) + i] for k in ks for i in range(1 if k < 8 else 2)]
        return jnp.concatenate(out, axis=1)

    def rows_of(weights, ks, j):
        cols = pl.ds(CW * j, CW)
        if list(ks) == list(range(ks[0], ks[0] + len(ks))):
            return weights[pl.ds(TILE * ks[0], TILE * len(ks)), cols]
        return jnp.concatenate([weights[pl.ds(TILE * k, TILE), cols] for k in ks], axis=0)

    def rec_dot(slot, ks, j):
        rows = jnp.concatenate([tiles_of(h8, h4, slot, ks), jnp.zeros((FILL, TILE * len(ks)), BF16)], axis=0)
        return jnp.dot(rows, rows_of(wrec, ks, j), preferred_element_type=F32)[:BATCH]

    def in_product(block, into, ks, half=None):
        used = ROWS if half is None else PAIR
        for j in range(NCHUNK):
            cols = pl.ds(CW * j, CW)
            if half is None:
                rows = tiles_of(a8, a4, block, ks)
            else:
                part_of = pl.ds(PAIR * half, PAIR)
                rows = tiles_of(a8.at[:, :, part_of], a4.at[:, :, part_of], block, ks)
                rows = jnp.concatenate([rows, jnp.zeros_like(rows)], axis=0)
            part = jnp.dot(rows, rows_of(win, ks, j), preferred_element_type=F32)[:used]
            if ks[0] == 0:
                zbuf[into, pl.ds(0, used), cols] = part + bias_s[0:1, cols]
            else:
                zbuf[into, pl.ds(0, used), cols] += part

    def put_h(slot, chunk, v):
        if chunk < 4:
            h8[slot, chunk // 2, :, pl.ds(LANES * (chunk % 2), LANES)] = v.astype(BF16)
        else:
            h4[slot, 0] = v.astype(BF16)

    def small_setup():
        for src_core in BOTH:
            for i, ref in enumerate((braw.at[src_core], hcraw.at[src_core, 0], hcraw.at[src_core, 1])):
                arrived(ref, small_recv.at[src_core, i])

        def get_bias(n):
            return jnp.broadcast_to(braw[n // 10, pl.ds(n % 10, 1), :], (8, LANES))

        def put_bias(n, v):
            bias_s[:, pl.ds(LANES * n, LANES)] = v

        _repack(get_bias, put_bias)
        for which in BOTH:
            def get(n):
                return hcraw[n // NCHUNK, which, :, pl.ds(LANES * (n % NCHUNK), LANES)]

            for chunk in range(NCHUNK):
                blocks = [10 * (u // 5) + u % 5 for u in (2 * chunk, 2 * chunk + 1)]
                v = jnp.where(col == 0, _halves(get, *blocks), _halves(get, *[n + 5 for n in blocks]))
                if which == 0:
                    put_h(TB - 1, chunk, v)
                else:
                    c_s[:, pl.ds(LANES * chunk, LANES)] = v

    def small_copies(layer, src_core, to):
        refs = (
            ((bias1, bias2)[layer], braw.at[src_core]),
            (h_first.at[layer], hcraw.at[src_core, 0]),
            (c_first.at[layer], hcraw.at[src_core, 1]),
        )
        out = []
        for i, (src, dst) in enumerate(refs):
            recv = small_recv.at[src_core, i]
            if to is None:
                out.append(pltpu.make_async_copy(src, dst, recv))
            else:
                out.append(remote(src, dst, small_send.at[i], recv, to))
        return out

    def split_units(get):
        near = [get(0), get(1), get(2)]
        a, b, c = (_roll_half(get(n)) for n in (2, 3, 4))
        return near, [jnp.where(_low_half(a), a, b), jnp.where(_low_half(b), b, c), c]

    def h_copy(slot, peer, part):
        to = PEERS[peer]
        rel = to[0] + 2 * to[2]
        if part < 2:
            src, dst = h8.at[slot, part], h8.at[slot, 2 * rel + part]
        else:
            src, dst = h4.at[slot, 0], h4.at[slot, rel]
        return remote(src, dst, h_send.at[slot], h_recv.at[slot, peer, part], to)

    def send_h(slot, part):
        queue = (
            ((DIAG, 0), (NEXT_X, 0), (NEXT_Y, 0)),
            ((DIAG, 1), (NEXT_Y, 1)),
            ((DIAG, 2), (NEXT_X, 1), (NEXT_X, 2), (NEXT_Y, 2)),
        )
        for peer, piece in queue[part]:
            h_copy(slot, peer, piece).start()

    def h_sent(slot):
        units_moved(3 * CHIP, h_send.at[slot])

    def pass_on(block, s, slot):
        rows = pl.ds(BATCH * s, BATCH)
        return (
            remote(h8.at[slot], a8.at[block, :, rows, :], d_send.at[slot], a_recv.at[2 * block + s // 2], PARTNER),
            remote(h4.at[slot], a4.at[block, :, rows, :], d_send.at[slot], a_recv.at[2 * block + s // 2], PARTNER),
        )

    def passed_on(slot):
        units_moved(HIDDEN, d_send.at[slot])

    def seq_pieces(block, i, send, hand_on):
        first, to = (1, ALONG) if hand_on else (0, ACROSS)
        bufs = ((a8, 4 * first + i, 4 + i), (a4, 2 * first + i, 2 + i))
        return [
            remote(buf.at[block, src], buf.at[block, dst], seq_send.at[send], a_recv.at[block], to)
            for buf, src, dst in bufs[: 2 if i < 2 else 1]
        ]

    def crosses_here(block):
        return lax.rem(block + col, 2) == 0

    def seq_step(b, s):
        ahead, behind = b + LEAD + 1, b + LEAD

        @pl.when(crosses_here(ahead) & (ahead < NBLK))
        def _():
            for cp in seq_pieces(jnp.minimum(ahead, NBLK - 1), s, s, False):
                cp.start()

        @pl.when(crosses_here(behind) & (behind < NBLK))
        def _():
            block = jnp.minimum(behind, NBLK - 1)
            if s == 0:
                block_arrived(block)
            for cp in seq_pieces(block, s, s, True):
                cp.start()

    def seq_sent(i, send):
        units_moved(TB * (TILE + LANES if i < 2 else TILE), seq_send.at[send])

    def block_arrived(block):
        units_moved(TB * HIDDEN // 2, a_recv.at[block])

    def wait_block(block):
        pl.when(jnp.logical_not(crosses_here(block)))(lambda: block_arrived(block))

    def pair_arrived(block, half):
        units_moved(2 * HIDDEN, a_recv.at[2 * block + half])

    def out_copies(block, ring):
        return (
            pltpu.make_async_copy(out_own.at[ring], h2_out.at[block], o_send.at[ring, 0]),
            remote(out_far.at[ring], h2_out.at[block], o_send.at[ring, 1], o_recv, PARTNER),
        )

    def out_wait(block, ring):
        own, far = out_copies(block, ring)
        own.wait()
        far.wait_send()

    def one_step(layer, b, s):
        prev = (s + TB - 1) % TB
        ring = lax.rem(b, 2)
        nxt = jnp.minimum(b + 1, NBLK - 1)
        rows = pl.ds(BATCH * s, BATCH)

        def wait_for(*parts):
            for peer, part in parts:
                h_copy(prev, peer, part).wait_recv()

        if s == TB - 1:
            h_sent(s)
        else:
            pl.when(b > 0)(lambda: h_sent(s))
        if layer == 0:
            if s == TB - 1:
                passed_on(0)
            else:
                pl.when(b > 0)(lambda: passed_on((s + 1) % TB))
        if layer == 1 and s == 0:
            pl.when(b > 1)(lambda: out_wait(jnp.maximum(b - 2, 0), ring))
        pair, odd = divmod(s, 2)
        from_z = zbuf.at[pair, pl.ds(BATCH * odd, BATCH)] if layer else zbuf.at[ring, rows]
        for j in range(NCHUNK):
            cols = pl.ds(CW * j, CW)
            z[:, cols] = from_z[:, cols] + rec_dot(prev, (0, 1), j)
        if layer:
            target = nxt if pair else b
            if s == 0:
                pair_arrived(b, 1)
            elif s == 2:
                pl.when(b + 1 < NBLK)(lambda: pair_arrived(nxt, 0))
            in_product(target, 1 - pair, HALVES[odd], 1 - pair)
        else:
            if s == 0:
                pl.when(b + 1 < NBLK)(lambda: wait_block(nxt))
            in_product(nxt, 1 - ring, SHARE[s])
        if layer == 0:
            seq_step(b, s)

        def add(*ks):
            for j in range(NCHUNK):
                z[:, pl.ds(CW * j, CW)] += rec_dot(prev, ks, j)

        wait_for((NEXT_Y, 0))
        add(4)
        wait_for((NEXT_X, 0), (NEXT_Y, 1))
        add(2, 5)
        wait_for((DIAG, 0), (NEXT_Y, 2), (NEXT_X, 1), (NEXT_X, 2), (DIAG, 1), (DIAG, 2))
        new, part = [], []

        def products(*chunks):
            for j in chunks:
                part.append(rec_dot(prev, (3, 6, 7, 8, 9), j))

        def cell(j):
            units = pl.ds(LANES * j, LANES)
            zj = z[:, pl.ds(CW * j, CW)] + part[j]
            gates = [zj[:, LANES * m : LANES * (m + 1)] for m in range(4)]
            c_new = _sigmoid(gates[1]) * c_s[:, units] + _sigmoid(gates[0]) * jnp.tanh(gates[2])
            c_s[:, units] = c_new
            h_new = _sigmoid(gates[3]) * jnp.tanh(c_new)
            new.append(h_new)
            put_h(s, j, h_new)

        products(0, 1, 2)
        cell(0)
        cell(1)
        send_h(s, 0)
        products(3, 4)
        cell(2)
        cell(3)
        send_h(s, 1)
        cell(4)
        send_h(s, 2)
        if layer == 0:
            if s == 0:
                @pl.when(b > 0)
                def _():
                    for cp in pass_on(jnp.maximum(b - 1, 0), TB - 1, prev):
                        cp.start()
            else:
                for cp in pass_on(b, s - 1, prev):
                    cp.start()
        if layer == 1:
            near, far = split_units(lambda n: new[n])
            for n in range(3):
                out_far[ring, rows, pl.ds(LANES * n, LANES)] = near[n].astype(BF16)
                out_own[ring, rows, pl.ds(LANES * n, LANES)] = far[n].astype(BF16)
            if s == TB - 1:
                for cp in out_copies(b, ring):
                    cp.start()

    def take_all(buf, layer, mat):
        for cross in BOTH:
            for src_core in (1, 0):
                take_weights(buf, layer == 1 or mat == 1, mat, cross, src_core)

    def run_layer(layer):
        def block(b, carry):
            if layer == 0:
                last = jnp.where(crosses_here(b + LEAD), NBLK - LEAD, NBLK - LEAD + 1)

                @pl.when((b > 0) & (b < last))
                def _():
                    for s in range(TB):
                        seq_sent(s, s)
            for s in range(TB):
                one_step(layer, b, s)
            return carry

        lax.fori_loop(0, NBLK, block, 0)

    def leave_exchange(layer):
        slot = TB - 1
        for peer in range(3):
            for part in range(3):
                h_copy(slot, peer, part).wait_recv()
        if layer == 0:
            for cp in pass_on(NBLK - 1, slot, slot):
                cp.start()
            for s in (1, 2, 3):
                passed_on(s)
        for s in range(TB):
            h_sent(s)

    def begin():
        small_setup()
        for part in range(3):
            send_h(TB - 1, part)

    def end(keep, give, out, other):
        parts = split_units(lambda n: c_s[:, pl.ds(LANES * n, LANES)])
        for i in BOTH:
            for n in range(3):
                hcraw[0, i, :, pl.ds(LANES * n, LANES)] = parts[i][n]
        wide = pl.ds(0, PAD)
        kept = pltpu.make_async_copy(hcraw.at[0, keep, :, wide], out, c_send.at[0])
        given = remote(hcraw.at[0, give, :, wide], out, c_send.at[1], c_recv, PARTNER)
        kept.start()
        given.start()
        kept.wait()
        given.wait_send()
        arrived(other, c_recv)

    def seq_copies(group, rel, to, sems):
        out = []
        for i in range(3):
            src = seq.at[:, :, pl.ds(TILE * i, TILE if i < 2 else REST)]
            dst = a8.at[:, 2 * rel + i] if i < 2 else a4.at[:, rel]
            if to is None:
                out.append(pltpu.make_async_copy(src, dst, seq_recv.at[rel, i]))
            else:
                out.append(remote(src, dst, sems[i], seq_recv.at[rel, i], to))
        return out

    @pl.when(core == 0)
    def _():
        local = seq_copies(0, 0, None, None)
        local += small_copies(0, 0, None)
        local += w_copies(0, False, 0, w_in1, 0, own_cols, win, None, 0)
        local += w_copies(1, True, 0, w_rec1, 0, own_cols, wrec, None, 0)
        sent = small_copies(1, 0, PARTNER)
        more = []
        for mat, ref, buf in ((0, w_in2, win), (1, w_rec2, wrec)):
            for half in BOTH:
                rows = pl.ds(half * UNIT, UNIT)
                if (mat, half) in DIRECT:
                    dst = buf.at[pl.ds(place(True, 1, 0, half, 0), UNIT), :]
                    recv = w_recv.at[mat, 1, 0, half, 0]
                    more.append(remote(ref.at[rows, far_cols], dst, st_send.at[mat, half], recv, OVER))
                else:
                    dst, recv = stage.at[mat, rows, :], st_recv.at[mat, half]
                    sent.append(remote(ref.at[rows, far_cols], dst, st_send.at[mat, half], recv, PARTNER))
        sent += w_copies(0, True, 0, w_in2, 0, own_cols, win, PARTNER, 4)
        sent += w_copies(1, True, 0, w_rec2, 0, own_cols, wrec, PARTNER, 6)
        cross_in = w_copies(0, False, 0, w_in1, 1, far_cols, win, ACROSS, 0)
        cross_rec = w_copies(1, True, 0, w_rec1, 1, far_cols, wrec, ACROSS, 2)
        for cp in cross_in + local + sent:
            cp.start()
        for rel in BOTH:
            for i in range(3):
                arrived(a8.at[:, 2 * rel + i] if i < 2 else a4.at[:, rel], seq_recv.at[rel, i])
        for n in BOTH:
            for i in range(TB):
                for cp in seq_pieces(col + 2 * n, i, TB * (n + 1) + i, False):
                    cp.start()
        for cp in cross_rec:
            cp.start()
        begin()
        for cp in more:
            cp.start()

        def hand_on(n):
            block_arrived(col + 2 * n)
            for i in range(TB):
                for cp in seq_pieces(col + 2 * n, i, TB * (n + 3) + i, True):
                    cp.start()

        hand_on(0)
        pl.when(col == 0)(lambda: hand_on(1))
        take_all(win, 0, 0)
        wait_block(0)
        for ks in SHARE:
            in_product(0, 0, ks)
        take_all(wrec, 0, 1)
        run_layer(0)
        leave_exchange(0)
        end(0, 1, c1_out, c2_out)
        arrived(h2_out, o_recv)
        for n in range(3):
            for i in range(TB):
                seq_sent(i, TB * (n + 1) + i)

        @pl.when(col == 0)
        def _():
            for i in range(TB):
                seq_sent(i, 4 * TB + i)

        for cp in sent + cross_in + cross_rec + more:
            cp.wait_send()

    @pl.when(core == 1)
    def _():
        local = small_copies(1, 1, None)
        local += w_copies(0, True, 1, w_in2, 0, own_cols, win, None, 0)
        local += w_copies(1, True, 1, w_rec2, 0, own_cols, wrec, None, 0)
        sent = seq_copies(0, 1, PARTNER, [small_send.at[3 + i] for i in range(3)])
        sent += small_copies(0, 1, PARTNER)
        sent += w_copies(0, False, 1, w_in1, 1, far_cols, win, OVER, 0)
        sent += w_copies(1, True, 1, w_rec1, 1, far_cols, wrec, OVER, 2)
        sent += w_copies(0, False, 1, w_in1, 0, own_cols, win, PARTNER, 4)
        sent += w_copies(1, True, 1, w_rec1, 0, own_cols, wrec, PARTNER, 6)
        late_rec = w_copies(1, True, 1, w_rec2, 1, far_cols, wrec, ACROSS, 10)
        for cp in sent + local:
            cp.start()
        late = w_copies(0, True, 1, w_in2, 1, far_cols, win, ACROSS, 8)
        for mat, buf, more in ((0, win, late_rec), (1, wrec, [])):
            for half in BOTH:
                if (mat, half) not in DIRECT:
                    rows = pl.ds(place(True, 1, 0, half, 0), UNIT)
                    src = stage.at[mat, pl.ds(half * UNIT, UNIT), :]
                    arrived(src, st_recv.at[mat, half])
                    recv = w_recv.at[mat, 1, 0, half, 0]
                    late.append(remote(src, buf.at[rows, :], fw_send.at[mat, half], recv, ACROSS))
            late += more
        for cp in late:
            cp.start()
        begin()
        take_all(win, 1, 0)
        pair_arrived(0, 0)
        for ks in HALVES:
            in_product(0, 0, ks, 0)
        take_all(wrec, 1, 1)
        run_layer(1)
        end(1, 0, c2_out, c1_out)
        for b in (NBLK - 2, NBLK - 1):
            out_wait(b, b % 2)
        leave_exchange(1)
        for cp in sent + late:
            cp.wait_send()


def _trim(c1_in, c2_in, c1_out, c2_out):
    c1_out[...] = c1_in[:, :UNIT]
    c2_out[...] = c2_in[:, :UNIT]


def solution(mesh):
    any_spec = pl.BlockSpec(memory_space=pl.ANY)
    dma = pltpu.SemaphoreType.DMA
    vmem = pltpu.VMEM

    def local_program(seq_in, w_in1, w_rec1, b_gate1, w_in2, w_rec2, b_gate2, h_init, c_init):
        seq = seq_in.reshape(NBLK, ROWS, CHIP)
        h2, c1, c2, _ = pl.pallas_call(
            _kernel,
            out_shape=(
                jax.ShapeDtypeStruct((NBLK, ROWS, PAD), BF16),
                jax.ShapeDtypeStruct((BATCH, PAD), F32),
                jax.ShapeDtypeStruct((BATCH, PAD), F32),
                jax.ShapeDtypeStruct((2, CHIP, GATES), BF16),
            ),
            in_specs=[any_spec] * 9,
            out_specs=(any_spec,) * 4,
            scratch_shapes=[
                vmem((HIDDEN, GATES), BF16),
                vmem((HIDDEN, GATES), BF16),
                vmem((NBLK, 8, ROWS, TILE), BF16),
                vmem((NBLK, 4, ROWS, LANES), BF16),
                vmem((2, ROWS, GATES), F32),
                vmem((BATCH, GATES), F32),
                vmem((TB, 8, BATCH, TILE), BF16),
                vmem((TB, 4, BATCH, LANES), BF16),
                vmem((BATCH, CHIP), F32),
                vmem((8, GATES), F32),
                vmem((2, 4 * UNIT // LANES, LANES), F32),
                vmem((2, 2, BATCH, CHIP), F32),
                vmem((2, ROWS, PAD), BF16),
                vmem((2, ROWS, PAD), BF16),
                vmem((TB * HIDDEN // 8, LANES), F32),
                dma((2, 2, 2, 2, 2)),
                dma((12, 2)),
                *[dma(SQUARE)] * 3,
                dma((2, 3)),
                dma((6,)),
                dma((2, 3)),
                dma((5 * TB,)),
                dma((2 * NBLK,)),
                dma((TB, 3, 3)),
                dma((TB,)),
                dma((TB,)),
                dma(()),
                dma(SQUARE),
                dma(()),
                dma((2,)),
            ],
            compiler_params=pltpu.CompilerParams(
                collective_id=0, has_side_effects=True, vmem_limit_bytes=62 * 2**20
            ),
        )(seq, w_in1, w_rec1, w_in2, w_rec2, b_gate1.reshape(-1, LANES), b_gate2.reshape(-1, LANES), h_init, c_init)
        cell = jax.ShapeDtypeStruct((BATCH, UNIT), F32)
        c1, c2 = pl.pallas_call(_trim, out_shape=(cell, cell))(c1, c2)
        return h2.reshape(STEPS, BATCH, PAD)[:, :, :UNIT], c1, c2

    row_spec = P(None, "dp", "row")
    weight_spec = P("row", "col")
    bias_spec = P(("col", "row"))
    seq_out_spec = P(None, "dp", ("row", "col"))
    cell_out_spec = P("dp", ("row", "col"))
    return jax.shard_map(
        local_program,
        mesh=mesh,
        in_specs=(row_spec, weight_spec, weight_spec, bias_spec, weight_spec, weight_spec, bias_spec, row_spec, row_spec),
        out_specs=(seq_out_spec, cell_out_spec, cell_out_spec),
        check_vma=False,
    )
```
